32 devices in a mesh: gx: 8 (over z, y), gy: 4 (over x, core).
Axes of the slice: x: 2, y: 2, z: 4, core: 2. Of those that a mesh axis runs over, the one named last changes fastest.
Arguments:
- block_list: int32 [64], P(('gx', 'gy')), may hold values from -1 to 63, as said below
- wet_levels: int32 [64, 1800], P(('gx', 'gy')), may hold values from 0 to 62, as said below
- mixing: float32 [64, 1800], P(('gx', 'gy')), may hold values from 0.5 to 2
- velocity: float32 [64, 2, 62, 1800], P(('gx', 'gy')), may hold values from -3 to 3
- tracers: float32 [64, 2, 62, 1800], P(('gx', 'gy')), may hold values from -6 to 6
- damping: float32 [160, 720], P('gy', 'gx'), may hold values from 0.05 to 0.5
Outputs:
- new_tracers: float32 [64, 2, 62, 1800], P(('gx', 'gy'))
- surface_height: float32 [160, 720], P('gy', 'gx')
The draws below stay inside these ranges and needn't reach their ends.
Inputs may be any that keep to these rules, and one draw needn't show every extreme that they name: `block_list`: slots form runs of 2 (run j holds slots j * 2 to j * 2 + 1). With q = j // 4 and r = j % 4, run j names distinct blocks r * 16 + q * 2 + s with 0 <= s < 2, in any order, and -1 in its remaining slots. Every run names one block or more, and the last run names all 2. Blocks that no run names are land. `wet_levels`: 0 in every slot whose block_list entry is -1; some column has 62 wet levels.
All inputs are finite; a program needn't handle non-finite values.
Results may differ from the reference program's by a relative error of at most 0.0003.
Values sent between devices are 32-bit elements; how exact they have to be, the bound alone decides.
A program may use at most 128 MiB of HBM per device.

```python
import math
import jax
import jax.numpy as jnp
from jax import lax

BX = 45
BY = 40
WATER_COLUMNS = 1800
VERTICAL_LEVELS = 62
TRACER_COUNT = 2
DEVICE_SLOTS = 2
PASSES = 2
ITERS = 3
GBX = 16
NY = 160
NX = 720
SLOT_TOTAL = 64


def layout(key):
    base_key = jax.random.fold_in(key, 4051)
    key_list = jax.random.split(base_key, 9)
    device_count = SLOT_TOTAL // DEVICE_SLOTS
    block_rows = NY // BY
    device_ids = jnp.arange(device_count, dtype=jnp.int32)
    live_counts = jax.random.randint(key_list[0], (device_count,), 1, DEVICE_SLOTS + 1)
    fullest = device_count - 1
    live_counts = jnp.where(device_ids == fullest, DEVICE_SLOTS, live_counts)
    scores = jax.random.randint(key_list[2], (device_count, DEVICE_SLOTS), 0, 1 << 20) * DEVICE_SLOTS + jnp.arange(DEVICE_SLOTS, dtype=jnp.int32)[None, :]
    ordering = jnp.argsort(scores, axis=1, stable=True).astype(jnp.int32)
    slot_ids = jnp.arange(DEVICE_SLOTS, dtype=jnp.int32)[None, :]
    present = slot_ids < live_counts[:, None]
    column_group = device_ids // block_rows
    row_group = device_ids % block_rows
    blocks = row_group[:, None] * GBX + column_group[:, None] * DEVICE_SLOTS + ordering
    block_listing = jnp.where(present, blocks, -1)
    depth_caps = jax.random.randint(key_list[3], (device_count,), VERTICAL_LEVELS // 4, VERTICAL_LEVELS + 1)
    deepest = jax.random.randint(key_list[4], (), 0, device_count)
    depth_caps = jnp.where(device_ids == deepest, VERTICAL_LEVELS, depth_caps)
    block_caps = 1 + jax.random.randint(key_list[5], (device_count, DEVICE_SLOTS), 0, 1 << 20) % depth_caps[:, None]
    block_caps = jnp.where(slot_ids == 0, depth_caps[:, None], block_caps)
    cell_ids = jnp.arange(WATER_COLUMNS, dtype=jnp.int32)[None, None, :]
    water_column_depth = 1 + jax.random.randint(key_list[6], (device_count, DEVICE_SLOTS, WATER_COLUMNS), 0, 1 << 20) % block_caps[:, :, None]
    deep_cell = jax.random.randint(key_list[7], (device_count, DEVICE_SLOTS, 1), 0, WATER_COLUMNS)
    dry_column = jax.random.randint(key_list[8], (device_count, DEVICE_SLOTS, WATER_COLUMNS), 0, 5) == 0
    water_column_depth = jnp.where(cell_ids == deep_cell, block_caps[:, :, None], jnp.where(dry_column, 0, water_column_depth))
    water_column_depth = jnp.where(present[:, :, None], water_column_depth, 0)
    return (block_listing.reshape(SLOT_TOTAL).astype(jnp.int32), water_column_depth.reshape(SLOT_TOTAL, WATER_COLUMNS).astype(jnp.int32))


def draw_block_list(key, part):
    return layout(key)[0]


def draw_wet_levels(key, part):
    return layout(key)[1]


def block_levels(rng, dims, cuts, low, high):
    def one(position, blocks):
        heights = jax.random.uniform(jax.random.fold_in(jax.random.fold_in(rng, 6), position), (blocks,), jnp.float32, low / len(cuts), high / len(cuts))
        return jnp.repeat(jnp.exp(heights), dims[position] // blocks).reshape((-1,) + (1,) * (len(dims) - position - 1))

    level = one(*cuts[0])
    for cut in cuts[1:]:
        level = level * one(*cut)
    return level


def scatter_about(rng, extent, deviation, reach, shards=(), kind=jnp.bfloat16):
    values = deviation * jax.random.normal(rng, extent, jnp.float32)
    if shards:
        values = values * block_levels(rng, extent, shards, -0.22, 0.18)
    return jnp.clip(values, -reach, reach).astype(kind)


def setup_inputs(seed: int = 0) -> dict:
    seeds = jax.random.split(jax.random.key(seed), 7)
    return {
        "block_list": draw_block_list(jax.random.fold_in(seeds[6], 71), 0),
        "wet_levels": draw_wet_levels(jax.random.fold_in(seeds[6], 71), 0),
        "mixing": jnp.clip(jnp.exp(math.log(2.0) - 1.3862944 * jax.random.uniform(seeds[2], (SLOT_TOTAL, WATER_COLUMNS), jnp.float32) ** block_levels(seeds[2], (SLOT_TOTAL, WATER_COLUMNS), ((0, 32),), -0.2, 0.2)), 0.5, 2.0),
        "velocity": scatter_about(seeds[3], (SLOT_TOTAL, 2, VERTICAL_LEVELS, WATER_COLUMNS), 0.5, 3.0, ((0, 32),), jnp.float32),
        "tracers": scatter_about(seeds[4], (SLOT_TOTAL, TRACER_COUNT, VERTICAL_LEVELS, WATER_COLUMNS), 1.0, 6.0, ((0, 32),), jnp.float32),
        "damping": jnp.clip(jnp.exp(math.log(0.5) - 2.3025851 * jax.random.uniform(seeds[5], (NY, NX), jnp.float32) ** block_levels(seeds[5], (NY, NX), ((0, 4), (1, 8)), -0.2, 0.2)), 0.05, 0.5),
    }


advect_rate = 0.25
mixing_rate = 0.015
salt_weight = 0.8
directions = ((0, 1), (0, -1), (1, 0), (-1, 0))

def window(values, shrink, step_y, step_x):
    height = values.shape[-2]
    breadth = values.shape[-1]
    return values[..., shrink + step_y:height - shrink + step_y, shrink + step_x:breadth - shrink + step_x]

def laplace(values, wetness, shrink):
    centre = window(values, shrink, 0, 0)
    wet_centre = window(wetness, shrink, 0, 0)
    pieces = [wet_centre * window(wetness, shrink, step_y, step_x) * (window(values, shrink, step_y, step_x) - centre) for step_y, step_x in directions]
    return pieces[0] + pieces[1] + pieces[2] + pieces[3]

def advect(values, wetness, eastward, northward):
    centre = window(values, 2, 0, 0)
    wet_centre = window(wetness, 2, 0, 0)

    def face_flux(speeds, step_y, step_x):
        face_speed = 0.5 * (window(speeds, 2, 0, 0) + window(speeds, 2, step_y, step_x))
        face_wet = wet_centre * window(wetness, 2, step_y, step_x)
        return face_wet * face_speed * (0.5 * (centre + window(values, 2, step_y, step_x)))
    return -(face_flux(eastward, 0, 1) - face_flux(eastward, 0, -1) + face_flux(northward, 1, 0) - face_flux(northward, -1, 0))

def tracer_pass(padded, wetness, eastward, northward, mixing):
    first_lap = laplace(padded, wetness, 1)
    scaled = window(mixing, 1, 0, 0) * first_lap
    biharmonic = -laplace(scaled, window(wetness, 1, 0, 0), 1)
    return window(padded, 2, 0, 0) + advect_rate * advect(padded, wetness, eastward, northward) + mixing_rate * biharmonic

def to_grid(slot_values, block_list):
    block_rows = NY // BY
    blocks = block_rows * GBX
    target = jnp.where(block_list >= 0, block_list, blocks).astype(jnp.int32)
    middle = slot_values.shape[1:-1]
    leading = len(middle)
    placed = jnp.zeros((blocks,) + middle + (WATER_COLUMNS,), slot_values.dtype).at[target].set(slot_values, mode='drop')
    placed = placed.reshape((block_rows, GBX) + middle + (BY, BX))
    axes_order = tuple(range(2, leading + 2)) + (0, leading + 2, 1, leading + 3)
    return placed.transpose(axes_order).reshape(middle + (NY, NX))

def from_grid(grid_values, block_list):
    block_rows = NY // BY
    middle = grid_values.shape[:-2]
    leading = len(middle)
    blocks = grid_values.reshape(middle + (block_rows, BY, GBX, BX))
    axes_order = (leading, leading + 2) + tuple(range(leading)) + (leading + 1, leading + 3)
    blocks = blocks.transpose(axes_order).reshape((block_rows * GBX,) + middle + (WATER_COLUMNS,))
    return blocks[jnp.maximum(block_list, 0).astype(jnp.int32)]

def pad_grid(values, margin):
    spacing = [(0, 0)] * (values.ndim - 2) + [(margin, margin), (0, 0)]
    padded_rows = jnp.pad(values, spacing)
    return jnp.concatenate([padded_rows[..., -margin:], padded_rows, padded_rows[..., :margin]], axis=-1)

def reference(block_list, wet_levels, mixing, velocity, tracers, damping):
    present = block_list >= 0
    depth_grid = to_grid(wet_levels.astype(jnp.float32), block_list)
    depth_pad = pad_grid(depth_grid, 2)
    mixing_pad = pad_grid(to_grid(mixing, block_list), 2)

    def level_step(forcing, level_index):
        level_tracers = lax.dynamic_index_in_dim(tracers, level_index, 2, keepdims=False)
        level_flow = lax.dynamic_index_in_dim(velocity, level_index, 2, keepdims=False)
        current = to_grid(level_tracers, block_list)
        flow_pad = pad_grid(to_grid(level_flow, block_list), 2)
        wetness = (level_index.astype(jnp.float32) < depth_pad).astype(jnp.float32)
        for pass_index in range(PASSES):
            current = tracer_pass(pad_grid(current, 2), wetness, flow_pad[0], flow_pad[1], mixing_pad)
        wet_inner = window(wetness, 2, 0, 0)
        forcing = forcing + wet_inner * (current[0] - salt_weight * current[1])
        return (forcing, from_grid(current, block_list))
    forcing, slot_levels = lax.scan(level_step, jnp.zeros((NY, NX), jnp.float32), jnp.arange(VERTICAL_LEVELS, dtype=jnp.int32))
    forcing = forcing / math.sqrt(VERTICAL_LEVELS)
    restored = jnp.transpose(slot_levels, (1, 2, 0, 3))
    new_tracers = jnp.where(present[:, None, None, None], restored, tracers)
    height_pad = pad_grid(depth_grid, 1)
    centre_depth = window(height_pad, 1, 0, 0)
    couplings = [jnp.minimum(centre_depth, window(height_pad, 1, step_y, step_x)) / VERTICAL_LEVELS for step_y, step_x in directions]
    diagonal = damping + (couplings[0] + couplings[1] + couplings[2] + couplings[3])

    def operate(values):
        padded = pad_grid(values, 1)
        beside = [couplings[number] * window(padded, 1, step_y, step_x) for number, (step_y, step_x) in enumerate(directions)]
        return diagonal * values - (beside[0] + beside[1] + beside[2] + beside[3])
    solution = jnp.zeros_like(forcing)
    residual = forcing
    direction = forcing
    norm_now = jnp.sum(residual * residual)
    for iteration in range(ITERS):
        applied = operate(direction)
        step_size = norm_now / jnp.sum(direction * applied)
        solution = solution + step_size * direction
        residual = residual - step_size * applied
        norm_next = jnp.sum(residual * residual)
        direction = residual + norm_next / norm_now * direction
        norm_now = norm_next
    return (new_tracers, solution)
```

```python
import functools
import math

import jax
import jax.numpy as jnp
from jax import lax
from jax.experimental import pallas as pl
from jax.experimental.pallas import tpu as pltpu
from jax.sharding import PartitionSpec as P

BX = 45
BY = 40
PASSES = 2
ITERS = 3

advect_rate = 0.25
mixing_rate = 0.015
salt_weight = 0.8

HALO = 4
X0 = 16
C0 = 8
HALF = 64
MESH = pl.DeviceIdType.MESH
CENTRE = 4.25
SPREAD = 4.25


def kernel(
    gx_count, gy_count, bl_ref, wet_ref, mix_ref, vel_ref, tr_ref, damp_ref, out_ref, sh_ref,
    tmp, cells, strip, adv, w_, u_, n_, m_, we, wn, ce, cn, g_, colsend, colrecv, corner,
    frame, sideframe, vertframe, redx, redy,
    col_sem, row_sem, corner_sem, side_sem, vert_sem, redx_sem, redy_sem,
):
    slots = tr_ref.shape[0]
    levels = tr_ref.shape[2]
    water = tr_ref.shape[3]
    span = slots * BX
    rows = BY + 2 * HALO
    chunks = water // 128
    tail = water - 128 * chunks
    width_vregs = (span + 2 * 4 + 6) // 8
    gx = lax.axis_index("gx")
    gy = lax.axis_index("gy")
    east = lax.rem(gx + 1, gx_count)
    west = lax.rem(gx + gx_count - 1, gx_count)
    has_n = gy < gy_count - 1
    has_s = gy > 0

    for a in range(2):
        for y in list(range(HALO)) + list(range(rows - HALO, rows)):
            strip[a, y] = jnp.zeros(strip.shape[2:], jnp.float32)

    barrier = pltpu.get_barrier_semaphore()
    for k in range(1, gx_count):
        pl.semaphore_signal(barrier, inc=1, device_id=(lax.rem(gx + k, gx_count), gy), device_id_type=MESH)
    for k in range(1, gy_count):
        pl.semaphore_signal(barrier, inc=1, device_id=(gx, lax.rem(gy + k, gy_count)), device_id_type=MESH)

    for side in (west, east):
        for step in (1, gy_count - 1):
            other = lax.rem(gy + step, gy_count)
            pl.semaphore_signal(barrier, inc=1, device_id=(side, other), device_id_type=MESH)

    where_slot = []
    for s in range(slots):
        b = bl_ref[s]
        where_slot.append(jnp.where(b >= 0, lax.rem(b, slots), -1))

    for t in range(4):
        tmp[t] = jnp.zeros((128, 128), jnp.float32)

    def chosen(p, pieces):
        value = jnp.zeros_like(pieces[0])
        for s in range(slots):
            value = jnp.where(where_slot[s] == p, pieces[s], value)
        return value

    def bring(cols, lanes):
        for p in range(slots):
            for a, ref in enumerate((vel_ref, tr_ref)):
                t = 2 * a + p
                for n in range(2):
                    tmp[t, HALF * n : HALF * n + levels, 0:lanes] = chosen(
                        p, [ref[s, n, :, cols] for s in range(slots)]
                    )
            tmp[p, levels : levels + 1, 0:lanes] = chosen(
                p, [wet_ref[s : s + 1, cols].astype(jnp.float32) for s in range(slots)]
            )
            tmp[p, HALF + levels : HALF + levels + 1, 0:lanes] = chosen(
                p, [mix_ref[s : s + 1, cols] for s in range(slots)]
            )

    def bring_chunk(j, carry):
        base = pl.multiple_of(j * 128, 128)
        bring(pl.ds(base, 128), 128)
        for t in range(4):
            cells[t, pl.ds(base, 128), :] = tmp[t].T
        return carry

    lax.fori_loop(0, chunks, bring_chunk, 0)
    bring(pl.ds(chunks * 128, tail), tail)
    for t in range(4):
        cells[t, chunks * 128 : chunks * 128 + 128, :] = tmp[t].T

    for a in range(2):
        for p in range(slots):
            for y in range(BY):
                strip[a, HALO + y, X0 + BX * p : X0 + BX * (p + 1), :] = cells[
                    2 * a + p, BX * y : BX * (y + 1), :
                ]

    for a in range(2):
        for y in range(BY):
            colsend[0, a, y] = strip[a, HALO + y, X0 : X0 + HALO, :]
            colsend[1, a, y] = strip[a, HALO + y, X0 + span - HALO : X0 + span, :]

    pl.semaphore_wait(barrier, gx_count - 1 + gy_count - 1 + 4)

    def remote(src, dst, sems, index, device):
        return pltpu.make_async_remote_copy(
            src_ref=src, dst_ref=dst, send_sem=sems.at[0, index], recv_sem=sems.at[1, index],
            device_id=device, device_id_type=MESH,
        )

    to_west = remote(colsend.at[0], colrecv.at[1], col_sem, 1, (west, gy))
    to_east = remote(colsend.at[1], colrecv.at[0], col_sem, 0, (east, gy))
    to_west.start()
    to_east.start()
    inner = pl.ds(X0, 96)
    to_north = remote(
        strip.at[:, pl.ds(BY, HALO), inner], strip.at[:, pl.ds(0, HALO), inner], row_sem, 0, (gx, gy + 1)
    )
    to_south = remote(
        strip.at[:, pl.ds(HALO, HALO), inner], strip.at[:, pl.ds(BY + HALO, HALO), inner], row_sem, 1, (gx, gy - 1)
    )

    @pl.when(has_n)
    def _():
        to_north.start()

    @pl.when(has_s)
    def _():
        to_south.start()

    to_west.wait()
    to_east.wait()

    def corner_copy(vert, side):
        source = colrecv.at[side, :, pl.ds(BY - HALO if vert == 0 else 0, HALO)]
        device = (gx, gy + 1) if vert == 0 else (gx, gy - 1)
        return remote(source, corner.at[vert, side], corner_sem, 2 * vert + side, device)

    @pl.when(has_n)
    def _():
        for side in range(2):
            corner_copy(0, side).start()

    @pl.when(has_s)
    def _():
        for side in range(2):
            corner_copy(1, side).start()

    @pl.when(has_n)
    def _():
        to_north.wait_send()
        for side in range(2):
            corner_copy(0, side).wait_send()

    @pl.when(has_s)
    def _():
        to_south.wait_send()
        for side in range(2):
            corner_copy(1, side).wait_send()

    @pl.when(has_s)
    def _():
        to_north.wait_recv()
        for side in range(2):
            corner_copy(0, side).wait_recv()

    @pl.when(has_n)
    def _():
        to_south.wait_recv()
        for side in range(2):
            corner_copy(1, side).wait_recv()

    halo_columns = ((X0 - HALO, X0), (X0 + span, X0 + span + HALO))
    for a in range(2):
        for side, (lo, hi) in enumerate(halo_columns):
            for y in range(BY):
                strip[a, HALO + y, lo:hi, :] = colrecv[side, a, y]

    def put_corners(vert):
        base = 0 if vert == 0 else HALO + BY
        for a in range(2):
            for side, (lo, hi) in enumerate(halo_columns):
                for y in range(HALO):
                    strip[a, base + y, lo:hi, :] = corner[vert, side, a, y]

    @pl.when(has_s)
    def _():
        put_corners(0)

    @pl.when(has_n)
    def _():
        put_corners(1)

    lane = lax.broadcasted_iota(jnp.int32, (8, 128), 1)
    low = lane < HALF
    level = jnp.where(low, lane, lane - HALF).astype(jnp.float32)

    def prepare(y, depths):
        kept = []
        for v in range(width_vregs):
            here = pl.ds(C0 + 8 * v, 8)
            flow = strip[0, y, here, :]
            depth = jnp.broadcast_to(flow[:, levels : levels + 1], (8, 128))
            mixing = jnp.broadcast_to(flow[:, HALF + levels : HALF + levels + 1], (8, 128))
            turned = pltpu.roll(flow, HALF, 1)
            w_[y, here, :] = jnp.where(level < depth, 1.0, 0.0)
            u_[y, here, :] = jnp.where(low, flow, turned)
            n_[y, here, :] = jnp.where(low, turned, flow)
            m_[y, here, :] = mixing_rate * mixing
            kept.append(jnp.where(lane == y, depth, depths[v]))
        return tuple(kept)

    blank = tuple(jnp.zeros((8, 128), jnp.float32) for _ in range(width_vregs))
    depth_columns = lax.fori_loop(0, rows, prepare, blank)

    def faces(y, carry):
        for v in range(width_vregs):
            x = C0 + 8 * v
            here = pl.ds(x, 8)
            there = pl.ds(x + 1, 8)
            wet = w_[y, here, :]
            wet_e = wet * w_[y, there, :]
            wet_n = wet * w_[y + 1, here, :]
            we[y, here, :] = wet_e
            wn[y, here, :] = wet_n
            scale = advect_rate * 0.25
            ce[y, here, :] = (scale * wet_e) * (u_[y, here, :] + u_[y, there, :])
            cn[y, here, :] = (scale * wet_n) * (n_[y, here, :] + n_[y + 1, here, :])
        return carry

    lax.fori_loop(0, rows - 1, faces, 0)

    def first(f, y, carry):
        for v in range(width_vregs):
            x = C0 + 8 * v
            here, right, left = pl.ds(x, 8), pl.ds(x + 1, 8), pl.ds(x - 1, 8)
            mid = f[y, here, :]
            lap = (
                we[y, here, :] * (f[y, right, :] - mid)
                + we[y, left, :] * (f[y, left, :] - mid)
                + wn[y, here, :] * (f[y + 1, here, :] - mid)
                + wn[y - 1, here, :] * (f[y - 1, here, :] - mid)
            )
            g_[y, here, :] = m_[y, here, :] * lap
        return carry

    def second(f, y, v):
        x = C0 + 8 * v
        here, right, left = pl.ds(x, 8), pl.ds(x + 1, 8), pl.ds(x - 1, 8)
        mid = f[y, here, :]
        gm = g_[y, here, :]
        flow = (
            ce[y, here, :] * (mid + f[y, right, :])
            - ce[y, left, :] * (mid + f[y, left, :])
            + cn[y, here, :] * (mid + f[y + 1, here, :])
            - cn[y - 1, here, :] * (mid + f[y - 1, here, :])
        )
        mix = (
            we[y, here, :] * (g_[y, right, :] - gm)
            + we[y, left, :] * (g_[y, left, :] - gm)
            + wn[y, here, :] * (g_[y + 1, here, :] - gm)
            + wn[y - 1, here, :] * (g_[y - 1, here, :] - gm)
        )
        return mid - (flow + mix)

    old, new = strip.at[1], adv
    lax.fori_loop(1, rows - 1, functools.partial(first, old), 0)

    def pass_one(y, carry):
        for v in range(width_vregs):
            adv[y, pl.ds(C0 + 8 * v, 8), :] = second(old, y, v)
        return carry

    lax.fori_loop(2, rows - 2, pass_one, 0)
    lax.fori_loop(3, rows - 3, functools.partial(first, new), 0)
    weight = jnp.where(low, 1.0, -salt_weight) * (1.0 / math.sqrt(levels))

    def pass_two(y, sums):
        kept = []
        for v in range(width_vregs):
            here = pl.ds(C0 + 8 * v, 8)
            value = second(new, y, v)
            strip[1, y, here, :] = value
            total = jnp.sum(w_[y, here, :] * weight * value, axis=1, keepdims=True)
            kept.append(jnp.where(lane == y, jnp.broadcast_to(total, (8, 128)), sums[v]))
        return tuple(kept)

    forcing_columns = lax.fori_loop(HALO, HALO + BY, pass_two, blank)

    def to_grid(columns, t):
        for v in range(width_vregs):
            tmp[t, 8 * v : 8 * v + 8, :] = columns[v]
        if width_vregs < 16:
            tmp[t, 8 * width_vregs : 128, :] = jnp.zeros((128 - 8 * width_vregs, 128), jnp.float32)
        return tmp[t].T[0:rows, :]

    frame[0] = to_grid(forcing_columns, 0)
    depth_grid = to_grid(depth_columns, 1)
    shift = X0 - C0
    tmp[2, HALO : HALO + BY, 0:span] = damp_ref[...]
    frame[1] = pltpu.roll(tmp[2, 0:rows, :], shift, 1)

    def side_copy(side):
        device = (east, gy) if side == 0 else (west, gy)
        return remote(frame, sideframe.at[side], side_sem, side, device)

    def vert_copy(vert, column):
        target = (east, gx, west)[column]
        source = frame.at[:, pl.ds(rows - 8 if vert == 0 else 0, 8)]
        device = (target, gy + 1) if vert == 0 else (target, gy - 1)
        return remote(source, vertframe.at[vert, column], vert_sem, 3 * vert + column, device)

    for side in range(2):
        side_copy(side).start()

    @pl.when(has_n)
    def _():
        for column in range(3):
            vert_copy(0, column).start()

    @pl.when(has_s)
    def _():
        for column in range(3):
            vert_copy(1, column).start()

    for p in range(slots):
        for y in range(BY):
            cells[p, BX * y : BX * (y + 1), :] = strip[1, HALO + y, X0 + BX * p : X0 + BX * (p + 1), :]

    def give(cols, lanes, base):
        turned = [cells[p, pl.ds(base, 128), :].T for p in range(slots)]
        for s in range(slots):
            for n in range(2):
                value = tr_ref[s, n, :, cols]
                for p in range(slots):
                    piece = turned[p][HALF * n : HALF * n + levels, 0:lanes]
                    value = jnp.where(where_slot[s] == p, piece, value)
                out_ref[s, n, :, cols] = value

    def give_chunk(j, carry):
        base = pl.multiple_of(j * 128, 128)
        give(pl.ds(base, 128), 128, base)
        return carry

    lax.fori_loop(0, chunks, give_chunk, 0)
    give(pl.ds(chunks * 128, tail), tail, chunks * 128)

    for side in range(2):
        side_copy(side).wait()

    @pl.when(has_n)
    def _():
        for column in range(3):
            vert_copy(0, column).wait_send()

    @pl.when(has_s)
    def _():
        for column in range(3):
            vert_copy(1, column).wait_send()

    @pl.when(has_s)
    def _():
        for column in range(3):
            vert_copy(0, column).wait_recv()

    @pl.when(has_n)
    def _():
        for column in range(3):
            vert_copy(1, column).wait_recv()

    lanes = lax.broadcasted_iota(jnp.int32, (rows, 128), 1)
    ys = lax.broadcasted_iota(jnp.int32, (rows, 128), 0)
    sub = lax.broadcasted_iota(jnp.int32, (8, 128), 0)

    def extended(kind):
        parts = []
        for column, middle in enumerate((sideframe.at[0, kind], frame.at[kind], sideframe.at[1, kind])):
            south = jnp.where(has_s, vertframe[0, column, kind], 0.0)
            north = jnp.where(has_n, vertframe[1, column, kind], 0.0)
            first_rows = jnp.where(sub < HALO, south, middle[0:8, :])
            last_rows = jnp.where(sub < HALO, middle[rows - 8 : rows, :], north)
            parts.append(jnp.concatenate([first_rows, middle[8 : rows - 8, :], last_rows], axis=0))
        return jnp.where(
            lanes < shift,
            pltpu.roll(parts[0], 128 - span, 1),
            jnp.where(lanes < shift + span, parts[1], pltpu.roll(parts[2], span, 1)),
        )

    forcing = extended(0)
    damping = extended(1)

    def nbr_e(v):
        return pltpu.roll(v, 127, 1)

    def nbr_w(v):
        return pltpu.roll(v, 1, 1)

    def nbr_n(v):
        return pltpu.roll(v, rows - 1, 0)

    def nbr_s(v):
        return pltpu.roll(v, 1, 0)

    hops = (nbr_e, nbr_w, nbr_n, nbr_s)
    couplings = [jnp.minimum(depth_grid, hop(depth_grid)) / levels for hop in hops]
    diagonal = damping + (couplings[0] + couplings[1] + couplings[2] + couplings[3]) - CENTRE

    def shifted(v):
        beside = [c * hop(v) for c, hop in zip(couplings, hops)]
        return (diagonal * v - (beside[0] + beside[1] + beside[2] + beside[3])) * (1.0 / SPREAD)

    basis = [forcing, shifted(forcing)]
    while len(basis) < ITERS + 1:
        basis.append(2.0 * shifted(basis[-1]) - basis[-2])
    inside = (ys >= HALO) & (ys < HALO + BY) & (lanes >= shift) & (lanes < shift + span)
    pairs = ((0, 0), (0, 1), (1, 1), (1, 2), (2, 2), (2, 3), (0, 2), (0, 3))
    for k, (i, j) in enumerate(pairs):
        product = jnp.where(inside, basis[i] * basis[j], 0.0)
        redx[0, k : k + 1, :] = jnp.sum(product, axis=0, keepdims=True)

    def redx_copy(k):
        return remote(redx.at[0], redx.at[k], redx_sem, k, (lax.rem(gx + k, gx_count), gy))

    def redy_copy(k):
        return remote(redy.at[0], redy.at[k], redy_sem, k, (gx, lax.rem(gy + k, gy_count)))

    for k in range(1, gx_count):
        redx_copy(k).start()
    for k in range(1, gx_count):
        redx_copy(k).wait()
    total = redx[0]
    for k in range(1, gx_count):
        total = total + redx[k]
    redy[0] = total
    for k in range(1, gy_count):
        redy_copy(k).start()
    for k in range(1, gy_count):
        redy_copy(k).wait()
    total = redy[0]
    for k in range(1, gy_count):
        total = total + redy[k]
    total = jnp.broadcast_to(jnp.sum(total, axis=1, keepdims=True), (8, 128))
    gram = {}
    for k, (i, j) in enumerate(pairs):
        gram[i, j] = gram[j, i] = total[k : k + 1, :]
    gram[1, 3] = gram[3, 1] = gram[2, 2] + gram[1, 1] - gram[0, 0]

    def inner_product(a, b):
        value = None
        for i, ai in enumerate(a):
            for j, bj in enumerate(b):
                if ai is not None and bj is not None:
                    term = ai * bj * gram[i, j]
                    value = term if value is None else value + term
        return value

    def add(a, b):
        return b if a is None else a if b is None else a + b

    def combine(a, scale, b):
        return [add(ai, None if bi is None else scale * bi) for ai, bi in zip(a, b)]

    def image_of(p):
        image = [None] * (ITERS + 1)
        for i in range(ITERS):
            if p[i] is None:
                continue
            image[i] = add(image[i], CENTRE * p[i])
            if i == 0:
                image[1] = add(image[1], SPREAD * p[i])
            else:
                image[i + 1] = add(image[i + 1], (0.5 * SPREAD) * p[i])
                image[i - 1] = add(image[i - 1], (0.5 * SPREAD) * p[i])
        return image

    one = jnp.ones((1, 128), jnp.float32)
    residual = [one] + [None] * ITERS
    direction = [one] + [None] * ITERS
    height = [None] * (ITERS + 1)
    norm = gram[0, 0]
    for iteration in range(ITERS):
        image = image_of(direction)
        step = norm / inner_product(direction, image)
        height = combine(height, step, direction)
        if iteration + 1 < ITERS:
            residual = combine(residual, -step, image)
            norm_next = inner_product(residual, residual)
            direction = combine(residual, norm_next / norm, direction)
            norm = norm_next
    answer = height[0] * basis[0] + height[1] * basis[1] + height[2] * basis[2]
    answer = pltpu.roll(pltpu.roll(answer, 128 - shift, 1), rows - HALO, 0)
    sh_ref[...] = answer[0:BY, 0:span]


def per_device(block_list, wet_levels, mixing, velocity, tracers, damping):
    gx_count = lax.axis_size("gx")
    gy_count = lax.axis_size("gy")
    slots = tracers.shape[0]
    span = slots * BX
    rows = BY + 2 * HALO
    wide = -(-(X0 + span + HALO + 8) // 8) * 8
    f32 = jnp.float32
    big = pltpu.VMEM((rows, wide, 128), f32)
    vmem = pl.BlockSpec(memory_space=pltpu.VMEM)
    dma = pltpu.SemaphoreType.DMA
    cell_rows = -(-tracers.shape[3] // 128) * 128
    return pl.pallas_call(
        functools.partial(kernel, gx_count, gy_count),
        out_shape=(
            jax.ShapeDtypeStruct(tracers.shape, f32),
            jax.ShapeDtypeStruct(damping.shape, f32),
        ),
        in_specs=[pl.BlockSpec(memory_space=pltpu.SMEM)] + [vmem] * 5,
        out_specs=(vmem, vmem),
        scratch_shapes=[
            pltpu.VMEM((4, 128, 128), f32),
            pltpu.VMEM((4, cell_rows, 128), f32),
            pltpu.VMEM((2, rows, wide, 128), f32),
            big, big, big, big, big, big, big, big, big, big,
            pltpu.VMEM((2, 2, BY, HALO, 128), f32),
            pltpu.VMEM((2, 2, BY, HALO, 128), f32),
            pltpu.VMEM((2, 2, 2, HALO, HALO, 128), f32),
            pltpu.VMEM((2, rows, 128), f32),
            pltpu.VMEM((2, 2, rows, 128), f32),
            pltpu.VMEM((2, 3, 2, 8, 128), f32),
            pltpu.VMEM((gx_count, 8, 128), f32),
            pltpu.VMEM((gy_count, 8, 128), f32),
            dma((2, 2)), dma((2, 2)), dma((2, 4)), dma((2, 2)), dma((2, 6)),
            dma((2, gx_count)), dma((2, gy_count)),
        ],
        compiler_params=pltpu.CompilerParams(
            collective_id=0, has_side_effects=True, vmem_limit_bytes=62 * 1024 * 1024
        ),
        name="ocean",
    )(block_list, wet_levels, mixing, velocity, tracers, damping)


def solution(mesh):
    return jax.shard_map(
        per_device,
        mesh=mesh,
        in_specs=(
            P(("gx", "gy")),
            P(("gx", "gy"), None),
            P(("gx", "gy"), None),
            P(("gx", "gy"), None, None, None),
            P(("gx", "gy"), None, None, None),
            P("gy", "gx"),
        ),
        out_specs=(P(("gx", "gy"), None, None, None), P("gy", "gx")),
        check_vma=False,
    )
```

```python
import functools
import math

import jax
import jax.numpy as jnp
from jax import lax
from jax.experimental import pallas as pl
from jax.experimental.pallas import tpu as pltpu
from jax.sharding import PartitionSpec as P

BX = 45
BY = 40
PASSES = 2
ITERS = 3

advect_rate = 0.25
mixing_rate = 0.015
salt_weight = 0.8

HALO = 4
X0 = 16
C0 = 8
HALF = 64
MESH = pl.DeviceIdType.MESH


def kernel(
    gx_count, gy_count, bl_ref, wet_ref, mix_ref, vel_ref, tr_ref, damp_ref, out_ref, sh_ref,
    tmp, cells, strip, adv, w_, u_, n_, m_, we, wn, ce, cn, g_, colsend, colrecv, corner,
    frame, sideframe, vertframe, redx, redy, fitx, fity, out_v,
    col_sem, row_sem, corner_sem, side_sem, vert_sem, redx_sem, redy_sem, fitx_sem, fity_sem, out_sem,
):
    slots = tr_ref.shape[0]
    levels = tr_ref.shape[2]
    water = tr_ref.shape[3]
    span = slots * BX
    rows = BY + 2 * HALO
    chunks = water // 128
    tail = water - 128 * chunks
    width_vregs = (span + 2 * 4 + 6) // 8
    gx = lax.axis_index("gx")
    gy = lax.axis_index("gy")
    east = lax.rem(gx + 1, gx_count)
    west = lax.rem(gx + gx_count - 1, gx_count)
    has_n = gy < gy_count - 1
    has_s = gy > 0

    for a in range(2):
        for y in list(range(HALO)) + list(range(rows - HALO, rows)):
            strip[a, y] = jnp.zeros(strip.shape[2:], jnp.float32)

    barrier = pltpu.get_barrier_semaphore()
    for k in range(1, gx_count):
        pl.semaphore_signal(barrier, inc=1, device_id=(lax.rem(gx + k, gx_count), gy), device_id_type=MESH)
    for k in range(1, gy_count):
        pl.semaphore_signal(barrier, inc=1, device_id=(gx, lax.rem(gy + k, gy_count)), device_id_type=MESH)

    for side in (west, east):
        for step in (1, gy_count - 1):
            other = lax.rem(gy + step, gy_count)
            pl.semaphore_signal(barrier, inc=1, device_id=(side, other), device_id_type=MESH)

    where_slot = []
    for s in range(slots):
        b = bl_ref[s]
        where_slot.append(jnp.where(b >= 0, lax.rem(b, slots), -1))

    for t in range(4):
        tmp[t] = jnp.zeros((128, 128), jnp.float32)

    def chosen(p, pieces):
        value = jnp.zeros_like(pieces[0])
        for s in range(slots):
            value = jnp.where(where_slot[s] == p, pieces[s], value)
        return value

    def remote(src, dst, sems, index, device):
        return pltpu.make_async_remote_copy(
            src_ref=src, dst_ref=dst, send_sem=sems.at[0, index], recv_sem=sems.at[1, index],
            device_id=device, device_id_type=MESH,
        )

    def bring(a, ref, cols, lanes):
        for p in range(slots):
            t = 2 * a + p
            for n in range(2):
                tmp[t, HALF * n : HALF * n + levels, 0:lanes] = chosen(
                    p, [ref[s, n, :, cols] for s in range(slots)]
                )
            if a == 0:
                tmp[p, levels : levels + 1, 0:lanes] = chosen(
                    p, [wet_ref[s : s + 1, cols].astype(jnp.float32) for s in range(slots)]
                )
                tmp[p, HALF + levels : HALF + levels + 1, 0:lanes] = chosen(
                    p, [mix_ref[s : s + 1, cols] for s in range(slots)]
                )

    def col_copy(a, side):
        device = (east, gy) if side == 0 else (west, gy)
        return remote(colsend.at[side, a], colrecv.at[side, a], col_sem, 2 * a + side, device)

    inner = pl.ds(X0, 96)

    def row_copy(a, vert):
        source = strip.at[a, pl.ds(BY if vert == 0 else HALO, HALO), inner]
        target = strip.at[a, pl.ds(0 if vert == 0 else BY + HALO, HALO), inner]
        return remote(source, target, row_sem, 2 * a + vert, (gx, gy + 1) if vert == 0 else (gx, gy - 1))

    def corner_copy(vert, side):
        source = colrecv.at[side, :, pl.ds(BY - HALO if vert == 0 else 0, HALO)]
        device = (gx, gy + 1) if vert == 0 else (gx, gy - 1)
        return remote(source, corner.at[vert, side], corner_sem, 2 * vert + side, device)

    def side_copy(kind, side):
        device = (east, gy) if side == 0 else (west, gy)
        return remote(frame.at[kind], sideframe.at[side, kind], side_sem, 2 * kind + side, device)

    def vert_copy(kind, vert, column):
        target = (east, gx, west)[column]
        source = frame.at[kind, pl.ds(rows - 8 if vert == 0 else 0, 8)]
        device = (target, gy + 1) if vert == 0 else (target, gy - 1)
        index = 6 * kind + 3 * vert + column
        return remote(source, vertframe.at[vert, column, kind], vert_sem, index, device)

    senders = (has_n, has_s)
    receivers = (has_s, has_n)

    for a, ref in enumerate((vel_ref, tr_ref)):

        def bring_chunk(j, carry):
            base = pl.multiple_of(j * 128, 128)
            bring(a, ref, pl.ds(base, 128), 128)
            for t in range(2 * a, 2 * a + 2):
                cells[t, pl.ds(base, 128), :] = tmp[t].T
            return carry

        lax.fori_loop(0, chunks, bring_chunk, 0)
        bring(a, ref, pl.ds(chunks * 128, tail), tail)
        for t in range(2 * a, 2 * a + 2):
            cells[t, chunks * 128 : chunks * 128 + 128, :] = tmp[t].T
        for p in range(slots):
            for y in range(BY):
                strip[a, HALO + y, X0 + BX * p : X0 + BX * (p + 1), :] = cells[
                    2 * a + p, BX * y : BX * (y + 1), :
                ]
        for y in range(BY):
            colsend[0, a, y] = strip[a, HALO + y, X0 + span - HALO : X0 + span, :]
            colsend[1, a, y] = strip[a, HALO + y, X0 : X0 + HALO, :]
        if a == 0:
            pl.semaphore_wait(barrier, gx_count - 1 + gy_count - 1 + 4)
        for side in range(2):
            col_copy(a, side).start()
        for vert in range(2):

            @pl.when(senders[vert])
            def _():
                row_copy(a, vert).start()

    shift = X0 - C0
    tmp[2, HALO : HALO + BY, 0:span] = damp_ref[...]
    frame[1] = pltpu.roll(tmp[2, 0:rows, :], shift, 1)

    def start_frames(kind):
        for side in range(2):
            side_copy(kind, side).start()
        for vert in range(2):

            @pl.when(senders[vert])
            def _():
                for column in range(3):
                    vert_copy(kind, vert, column).start()

    def wait_frames(kind):
        for side in range(2):
            side_copy(kind, side).wait()
        for vert in range(2):

            @pl.when(senders[vert])
            def _():
                for column in range(3):
                    vert_copy(kind, vert, column).wait_send()

            @pl.when(receivers[vert])
            def _():
                for column in range(3):
                    vert_copy(kind, vert, column).wait_recv()

    start_frames(1)

    halo_columns = ((X0 - HALO, X0), (X0 + span, X0 + span + HALO))

    def put_columns():
        for a in range(2):
            for side, (lo, hi) in enumerate(halo_columns):
                for y in range(BY):
                    strip[a, HALO + y, lo:hi, :] = colrecv[side, a, y]

    def put_corners(vert):
        base = 0 if vert == 0 else HALO + BY
        for a in range(2):
            for side, (lo, hi) in enumerate(halo_columns):
                for y in range(HALO):
                    strip[a, base + y, lo:hi, :] = corner[vert, side, a, y]

    lane = lax.broadcasted_iota(jnp.int32, (8, 128), 1)
    low = lane < HALF
    level = jnp.where(low, lane, lane - HALF).astype(jnp.float32)

    def prepare(tiles, y, depths):
        kept = list(depths)
        for v in tiles:
            here = pl.ds(C0 + 8 * v, 8)
            flow = strip[0, y, here, :]
            depth = jnp.broadcast_to(flow[:, levels : levels + 1], (8, 128))
            mixing = jnp.broadcast_to(flow[:, HALF + levels : HALF + levels + 1], (8, 128))
            turned = pltpu.roll(flow, HALF, 1)
            w_[y, here, :] = jnp.where(level < depth, 1.0, 0.0)
            u_[y, here, :] = jnp.where(low, flow, turned)
            n_[y, here, :] = jnp.where(low, turned, flow)
            m_[y, here, :] = mixing_rate * mixing
            kept[v] = jnp.where(lane == y, depth, depths[v])
        return tuple(kept)

    blank = tuple(jnp.zeros((8, 128), jnp.float32) for _ in range(width_vregs))

    def faces(tiles, y, carry):
        for v in tiles:
            x = C0 + 8 * v
            here = pl.ds(x, 8)
            there = pl.ds(x + 1, 8)
            wet = w_[y, here, :]
            wet_e = wet * w_[y, there, :]
            wet_n = wet * w_[y + 1, here, :]
            we[y, here, :] = wet_e
            wn[y, here, :] = wet_n
            scale = advect_rate * 0.25
            ce[y, here, :] = (scale * wet_e) * (u_[y, here, :] + u_[y, there, :])
            cn[y, here, :] = (scale * wet_n) * (n_[y, here, :] + n_[y + 1, here, :])
        return carry

    def first(f, tiles, y, carry):
        for v in tiles:
            x = C0 + 8 * v
            here, right, left = pl.ds(x, 8), pl.ds(x + 1, 8), pl.ds(x - 1, 8)
            mid = f[y, here, :]
            lap = (
                we[y, here, :] * (f[y, right, :] - mid)
                + we[y, left, :] * (f[y, left, :] - mid)
                + wn[y, here, :] * (f[y + 1, here, :] - mid)
                + wn[y - 1, here, :] * (f[y - 1, here, :] - mid)
            )
            g_[y, here, :] = m_[y, here, :] * lap
        return carry

    def second(f, y, v):
        x = C0 + 8 * v
        here, right, left = pl.ds(x, 8), pl.ds(x + 1, 8), pl.ds(x - 1, 8)
        mid = f[y, here, :]
        gm = g_[y, here, :]
        flow = (
            ce[y, here, :] * (mid + f[y, right, :])
            - ce[y, left, :] * (mid + f[y, left, :])
            + cn[y, here, :] * (mid + f[y + 1, here, :])
            - cn[y - 1, here, :] * (mid + f[y - 1, here, :])
        )
        mix = (
            we[y, here, :] * (g_[y, right, :] - gm)
            + we[y, left, :] * (g_[y, left, :] - gm)
            + wn[y, here, :] * (g_[y + 1, here, :] - gm)
            + wn[y - 1, here, :] * (g_[y - 1, here, :] - gm)
        )
        return mid - (flow + mix)

    old, new = strip.at[1], adv

    def pass_one(tiles, y, carry):
        for v in tiles:
            adv[y, pl.ds(C0 + 8 * v, 8), :] = second(old, y, v)
        return carry

    every = range(width_vregs)

    def early(step, bounds, tiles, carry=0):
        return lax.fori_loop(bounds[0], bounds[1], functools.partial(step, tiles), carry)

    def late(step, outer, bounds, tiles, carry=0):
        rest = [v for v in every if v not in tiles]
        carry = lax.fori_loop(outer[0], bounds[0], functools.partial(step, every), carry)
        carry = lax.fori_loop(bounds[1], outer[1], functools.partial(step, every), carry)
        return lax.fori_loop(bounds[0], bounds[1], functools.partial(step, rest), carry)

    last = rows - HALO
    full = span // 8
    step_one = functools.partial(first, old)
    depth_columns = early(prepare, (HALO, last), range(1, full + 1), blank)
    early(faces, (HALO, last - 1), range(1, full))
    for a in range(2):
        for side in range(2):
            col_copy(a, side).wait()
    for vert in range(2):

        @pl.when(senders[vert])
        def _():
            for side in range(2):
                corner_copy(vert, side).start()

    early(step_one, (HALO + 1, last - 1), range(2, full))
    early(pass_one, (HALO + 2, last - 2), range(3, full - 1))

    for vert in range(2):

        @pl.when(senders[vert])
        def _():
            for a in range(2):
                row_copy(a, vert).wait_send()
            for side in range(2):
                corner_copy(vert, side).wait_send()

        @pl.when(receivers[vert])
        def _():
            for a in range(2):
                row_copy(a, vert).wait_recv()
            for side in range(2):
                corner_copy(vert, side).wait_recv()

    put_columns()
    for vert in range(2):

        @pl.when(receivers[vert])
        def _():
            put_corners(vert)

    depth_columns = late(prepare, (0, rows), (HALO, last), range(1, full + 1), depth_columns)

    lanes = lax.broadcasted_iota(jnp.int32, (rows, 128), 1)
    ys = lax.broadcasted_iota(jnp.int32, (rows, 128), 0)
    sub = lax.broadcasted_iota(jnp.int32, (8, 128), 0)
    inside = (ys >= HALO) & (ys < HALO + BY) & (lanes >= shift) & (lanes < shift + span)

    def nbr_e(v):
        return pltpu.roll(v, 127, 1)

    def nbr_w(v):
        return pltpu.roll(v, 1, 1)

    def nbr_n(v):
        return pltpu.roll(v, rows - 1, 0)

    def nbr_s(v):
        return pltpu.roll(v, 1, 0)

    hops = (nbr_e, nbr_w, nbr_n, nbr_s)

    def to_grid(columns, t):
        for v in range(width_vregs):
            tmp[t, 8 * v : 8 * v + 8, :] = columns[v]
        if width_vregs < 16:
            tmp[t, 8 * width_vregs : 128, :] = jnp.zeros((128 - 8 * width_vregs, 128), jnp.float32)
        return tmp[t].T[0:rows, :]

    def pack(products):
        columns = [jnp.sum(jnp.where(inside, p, 0.0), axis=0, keepdims=True) for p in products]
        row = jnp.zeros((1, 128), jnp.float32)
        place = lax.broadcasted_iota(jnp.int32, (1, 128), 1)
        for k, column in enumerate(columns):
            row = jnp.where(place == k, jnp.sum(column, axis=1, keepdims=True), row)
        return row

    def x_copy(buffer, sems, k):
        return remote(buffer.at[0], buffer.at[k], sems, k, (lax.rem(gx + k, gx_count), gy))

    def y_copy(buffer, sems, k):
        return remote(buffer.at[0], buffer.at[k], sems, k, (gx, lax.rem(gy + k, gy_count)))

    def start_sum(copy, buffer, sems, row):
        buffer[0] = row
        for k in range(1, buffer.shape[0]):
            copy(buffer, sems, k).start()

    def end_sum(copy, buffer, sems):
        for k in range(1, buffer.shape[0]):
            copy(buffer, sems, k).wait()
        total = buffer[0]
        for k in range(1, buffer.shape[0]):
            total = total + buffer[k]
        return total

    depth_grid = to_grid(depth_columns, 1)
    couplings = [jnp.minimum(depth_grid, hop(depth_grid)) / levels for hop in hops]
    coupled = couplings[0] + couplings[1] + couplings[2] + couplings[3]
    squares = sum(c * c for c in couplings)
    own = frame[1] + coupled
    start_sum(
        x_copy, fitx, fitx_sem,
        pack([depth_grid, depth_grid * own, depth_grid * (own * own + squares)]),
    )

    late(faces, (0, rows - 1), (HALO, last - 1), range(1, full))
    late(step_one, (1, rows - 1), (HALO + 1, last - 1), range(2, full))
    late(pass_one, (2, rows - 2), (HALO + 2, last - 2), range(3, full - 1))
    start_sum(y_copy, fity, fity_sem, end_sum(x_copy, fitx, fitx_sem))
    lax.fori_loop(3, rows - 3, functools.partial(first, new, every), 0)
    weight = jnp.where(low, 1.0, -salt_weight) * (1.0 / math.sqrt(levels))

    def pass_two(y, sums):
        kept = []
        for v in range(width_vregs):
            here = pl.ds(C0 + 8 * v, 8)
            value = second(new, y, v)
            strip[1, y, here, :] = value
            total = jnp.sum(w_[y, here, :] * weight * value, axis=1, keepdims=True)
            kept.append(jnp.where(lane == y, jnp.broadcast_to(total, (8, 128)), sums[v]))
        return tuple(kept)

    forcing_columns = lax.fori_loop(HALO, HALO + BY, pass_two, blank)

    frame[0] = to_grid(forcing_columns, 0)
    start_frames(0)

    fit = end_sum(y_copy, fity, fity_sem)
    centre = fit[:, 1:2] / fit[:, 0:1]
    variance = fit[:, 2:3] / fit[:, 0:1] - centre * centre
    spread = jnp.maximum(2.0 * jnp.sqrt(jnp.maximum(variance, 0.0)), 0.1 * centre)
    centre = jnp.broadcast_to(centre, (1, 128))
    spread = jnp.broadcast_to(spread, (1, 128))

    for p in range(slots):
        for y in range(BY):
            cells[p, BX * y : BX * (y + 1), :] = strip[1, HALO + y, X0 + BX * p : X0 + BX * (p + 1), :]

    def give(cols, lanes, base):
        turned = [cells[p, pl.ds(base, 128), :].T for p in range(slots)]
        for s in range(slots):
            for n in range(2):
                value = tr_ref[s, n, :, cols]
                for p in range(slots):
                    piece = turned[p][HALF * n : HALF * n + levels, 0:lanes]
                    value = jnp.where(where_slot[s] == p, piece, value)
                out_v[s, n, :, cols] = value

    def give_chunk(j, carry):
        base = pl.multiple_of(j * 128, 128)
        give(pl.ds(base, 128), 128, base)
        return carry

    lax.fori_loop(0, chunks, give_chunk, 0)
    give(pl.ds(chunks * 128, tail), tail, chunks * 128)
    out_copy = pltpu.make_async_copy(out_v, out_ref, out_sem)
    out_copy.start()

    wait_frames(1)
    wait_frames(0)

    def extended(kind):
        parts = []
        for column, middle in enumerate((sideframe.at[0, kind], frame.at[kind], sideframe.at[1, kind])):
            south = jnp.where(has_s, vertframe[0, column, kind], 0.0)
            north = jnp.where(has_n, vertframe[1, column, kind], 0.0)
            first_rows = jnp.where(sub < HALO, south, middle[0:8, :])
            last_rows = jnp.where(sub < HALO, middle[rows - 8 : rows, :], north)
            parts.append(jnp.concatenate([first_rows, middle[8 : rows - 8, :], last_rows], axis=0))
        return jnp.where(
            lanes < shift,
            pltpu.roll(parts[0], 128 - span, 1),
            jnp.where(lanes < shift + span, parts[1], pltpu.roll(parts[2], span, 1)),
        )

    forcing = extended(0)
    damping = extended(1)

    diagonal = damping + coupled - centre

    def shifted(v):
        beside = [c * hop(v) for c, hop in zip(couplings, hops)]
        return (diagonal * v - (beside[0] + beside[1] + beside[2] + beside[3])) / spread

    basis = [forcing, shifted(forcing)]
    while len(basis) < ITERS + 1:
        basis.append(2.0 * shifted(basis[-1]) - basis[-2])
    pairs = ((0, 0), (0, 1), (1, 1), (1, 2), (2, 2), (2, 3), (0, 2), (0, 3), (1, 3))
    start_sum(x_copy, redx, redx_sem, pack([basis[i] * basis[j] for i, j in pairs]))
    start_sum(y_copy, redy, redy_sem, end_sum(x_copy, redx, redx_sem))
    total = end_sum(y_copy, redy, redy_sem)
    gram = {}
    for k, (i, j) in enumerate(pairs):
        gram[i, j] = gram[j, i] = jnp.broadcast_to(total[:, k : k + 1], (1, 128))

    def inner_product(a, b):
        value = None
        for i, ai in enumerate(a):
            for j, bj in enumerate(b):
                if ai is not None and bj is not None:
                    term = ai * bj * gram[i, j]
                    value = term if value is None else value + term
        return value

    def add(a, b):
        return b if a is None else a if b is None else a + b

    def combine(a, scale, b):
        return [add(ai, None if bi is None else scale * bi) for ai, bi in zip(a, b)]

    def image_of(p):
        image = [None] * (ITERS + 1)
        for i in range(ITERS):
            if p[i] is None:
                continue
            image[i] = add(image[i], centre * p[i])
            if i == 0:
                image[1] = add(image[1], spread * p[i])
            else:
                image[i + 1] = add(image[i + 1], (0.5 * spread) * p[i])
                image[i - 1] = add(image[i - 1], (0.5 * spread) * p[i])
        return image

    one = jnp.ones((1, 128), jnp.float32)
    residual = [one] + [None] * ITERS
    direction = [one] + [None] * ITERS
    height = [None] * (ITERS + 1)
    norm = gram[0, 0]
    for iteration in range(ITERS):
        image = image_of(direction)
        step = norm / inner_product(direction, image)
        height = combine(height, step, direction)
        if iteration + 1 < ITERS:
            residual = combine(residual, -step, image)
            norm_next = inner_product(residual, residual)
            direction = combine(residual, norm_next / norm, direction)
            norm = norm_next
    answer = height[0] * basis[0] + height[1] * basis[1] + height[2] * basis[2]
    answer = pltpu.roll(pltpu.roll(answer, 128 - shift, 1), rows - HALO, 0)
    sh_ref[...] = answer[0:BY, 0:span]
    out_copy.wait()


def per_device(block_list, wet_levels, mixing, velocity, tracers, damping):
    gx_count = lax.axis_size("gx")
    gy_count = lax.axis_size("gy")
    slots = tracers.shape[0]
    span = slots * BX
    rows = BY + 2 * HALO
    wide = -(-(X0 + span + HALO + 8) // 8) * 8
    f32 = jnp.float32
    big = pltpu.VMEM((rows, wide, 128), f32)
    vmem = pl.BlockSpec(memory_space=pltpu.VMEM)
    dma = pltpu.SemaphoreType.DMA
    cell_rows = -(-tracers.shape[3] // 128) * 128
    return pl.pallas_call(
        functools.partial(kernel, gx_count, gy_count),
        out_shape=(
            jax.ShapeDtypeStruct(tracers.shape, f32),
            jax.ShapeDtypeStruct(damping.shape, f32),
        ),
        in_specs=[pl.BlockSpec(memory_space=pltpu.SMEM)] + [vmem] * 5,
        out_specs=(pl.BlockSpec(memory_space=pl.ANY), vmem),
        scratch_shapes=[
            pltpu.VMEM((4, 128, 128), f32),
            pltpu.VMEM((4, cell_rows, 128), f32),
            pltpu.VMEM((2, rows, wide, 128), f32),
            big, big, big, big, big, big, big, big, big, big,
            pltpu.VMEM((2, 2, BY, HALO, 128), f32),
            pltpu.VMEM((2, 2, BY, HALO, 128), f32),
            pltpu.VMEM((2, 2, 2, HALO, HALO, 128), f32),
            pltpu.VMEM((2, rows, 128), f32),
            pltpu.VMEM((2, 2, rows, 128), f32),
            pltpu.VMEM((2, 3, 2, 8, 128), f32),
            pltpu.VMEM((gx_count, 1, 128), f32),
            pltpu.VMEM((gy_count, 1, 128), f32),
            pltpu.VMEM((gx_count, 1, 128), f32),
            pltpu.VMEM((gy_count, 1, 128), f32),
            pltpu.VMEM(tracers.shape, f32),
            dma((2, 4)), dma((2, 4)), dma((2, 4)), dma((2, 4)), dma((2, 12)),
            dma((2, gx_count)), dma((2, gy_count)), dma((2, gx_count)), dma((2, gy_count)), dma,
        ],
        compiler_params=pltpu.CompilerParams(
            collective_id=0, has_side_effects=True, vmem_limit_bytes=62 * 1024 * 1024
        ),
        name="ocean",
    )(block_list, wet_levels, mixing, velocity, tracers, damping)


def solution(mesh):
    return jax.shard_map(
        per_device,
        mesh=mesh,
        in_specs=(
            P(("gx", "gy")),
            P(("gx", "gy"), None),
            P(("gx", "gy"), None),
            P(("gx", "gy"), None, None, None),
            P(("gx", "gy"), None, None, None),
            P("gy", "gx"),
        ),
        out_specs=(P(("gx", "gy"), None, None, None), P("gy", "gx")),
        check_vma=False,
    )
```

```python
import functools
import math

import jax
import jax.numpy as jnp
from jax import lax
from jax.experimental import pallas as pl
from jax.experimental.pallas import tpu as pltpu
from jax.sharding import PartitionSpec as P

BX = 45
BY = 40
PASSES = 2
ITERS = 3

advect_rate = 0.25
mixing_rate = 0.015
salt_weight = 0.8

HALO = 4
X0 = 16
C0 = 8
HALF = 64
MESH = pl.DeviceIdType.MESH


def kernel(
    gx_count, gy_count, bl_ref, wet_ref, mix_ref, vel_ref, tr_ref, damp_ref, out_ref, sh_ref,
    tmp, cells, strip, adv, w_, u_, n_, m_, we, wn, ce, cn, g_, colsend, colrecv, corner,
    frame, sideframe, vertframe, redx, redy, fitx, fity, out_v,
    col_sem, row_sem, corner_sem, side_sem, vert_sem, redx_sem, redy_sem, fitx_sem, fity_sem, out_sem,
):
    slots = tr_ref.shape[0]
    levels = tr_ref.shape[2]
    water = tr_ref.shape[3]
    span = slots * BX
    rows = BY + 2 * HALO
    chunks = water // 128
    tail = water - 128 * chunks
    width_vregs = (span + 2 * 4 + 6) // 8
    gx = lax.axis_index("gx")
    gy = lax.axis_index("gy")
    east = lax.rem(gx + 1, gx_count)
    west = lax.rem(gx + gx_count - 1, gx_count)
    has_n = gy < gy_count - 1
    has_s = gy > 0

    for a in range(2):
        for y in list(range(HALO)) + list(range(rows - HALO, rows)):
            strip[a, y] = jnp.zeros(strip.shape[2:], jnp.float32)

    barrier = pltpu.get_barrier_semaphore()
    for k in range(1, gx_count):
        pl.semaphore_signal(barrier, inc=1, device_id=(lax.rem(gx + k, gx_count), gy), device_id_type=MESH)
    for k in range(1, gy_count):
        pl.semaphore_signal(barrier, inc=1, device_id=(gx, lax.rem(gy + k, gy_count)), device_id_type=MESH)

    for side in (west, east):
        for step in (1, gy_count - 1):
            other = lax.rem(gy + step, gy_count)
            pl.semaphore_signal(barrier, inc=1, device_id=(side, other), device_id_type=MESH)

    where_slot = []
    for s in range(slots):
        b = bl_ref[s]
        where_slot.append(jnp.where(b >= 0, lax.rem(b, slots), -1))

    for t in range(4):
        tmp[t] = jnp.zeros((128, 128), jnp.float32)

    def chosen(p, pieces):
        value = jnp.zeros_like(pieces[0])
        for s in range(slots):
            value = jnp.where(where_slot[s] == p, pieces[s], value)
        return value

    def remote(src, dst, sems, index, device):
        return pltpu.make_async_remote_copy(
            src_ref=src, dst_ref=dst, send_sem=sems.at[0, index], recv_sem=sems.at[1, index],
            device_id=device, device_id_type=MESH,
        )

    def bring(a, ref, cols, lanes):
        for p in range(slots):
            t = 2 * a + p
            for n in range(2):
                tmp[t, HALF * n : HALF * n + levels, 0:lanes] = chosen(
                    p, [ref[s, n, :, cols] for s in range(slots)]
                )
            if a == 0:
                tmp[p, levels : levels + 1, 0:lanes] = chosen(
                    p, [wet_ref[s : s + 1, cols].astype(jnp.float32) for s in range(slots)]
                )
                tmp[p, HALF + levels : HALF + levels + 1, 0:lanes] = chosen(
                    p, [mix_ref[s : s + 1, cols] for s in range(slots)]
                )

    def col_copy(a, side):
        device = (east, gy) if side == 0 else (west, gy)
        return remote(colsend.at[side, a], colrecv.at[side, a], col_sem, 2 * a + side, device)

    inner = pl.ds(X0, 96)

    def row_copy(a, vert):
        source = strip.at[a, pl.ds(BY if vert == 0 else HALO, HALO), inner]
        target = strip.at[a, pl.ds(0 if vert == 0 else BY + HALO, HALO), inner]
        return remote(source, target, row_sem, 2 * a + vert, (gx, gy + 1) if vert == 0 else (gx, gy - 1))

    def corner_copy(vert, side):
        source = colrecv.at[side, :, pl.ds(BY - HALO if vert == 0 else 0, HALO)]
        device = (gx, gy + 1) if vert == 0 else (gx, gy - 1)
        return remote(source, corner.at[vert, side], corner_sem, 2 * vert + side, device)

    def side_copy(kind, side):
        device = (east, gy) if side == 0 else (west, gy)
        return remote(frame.at[kind], sideframe.at[side, kind], side_sem, 2 * kind + side, device)

    def vert_copy(kind, vert, column):
        target = (east, gx, west)[column]
        source = frame.at[kind, pl.ds(rows - 8 if vert == 0 else 0, 8)]
        device = (target, gy + 1) if vert == 0 else (target, gy - 1)
        index = 6 * kind + 3 * vert + column
        return remote(source, vertframe.at[vert, column, kind], vert_sem, index, device)

    senders = (has_n, has_s)
    receivers = (has_s, has_n)

    for a, ref in enumerate((vel_ref, tr_ref)):

        def bring_chunk(j, carry):
            base = pl.multiple_of(j * 128, 128)
            bring(a, ref, pl.ds(base, 128), 128)
            for t in range(2 * a, 2 * a + 2):
                cells[t, pl.ds(base, 128), :] = tmp[t].T
            return carry

        lax.fori_loop(0, chunks, bring_chunk, 0)
        bring(a, ref, pl.ds(chunks * 128, tail), tail)
        for t in range(2 * a, 2 * a + 2):
            cells[t, chunks * 128 : chunks * 128 + 128, :] = tmp[t].T
        for p in range(slots):
            for y in range(BY):
                strip[a, HALO + y, X0 + BX * p : X0 + BX * (p + 1), :] = cells[
                    2 * a + p, BX * y : BX * (y + 1), :
                ]
        for y in range(BY):
            colsend[0, a, y] = strip[a, HALO + y, X0 + span - HALO : X0 + span, :]
            colsend[1, a, y] = strip[a, HALO + y, X0 : X0 + HALO, :]
        if a == 0:
            pl.semaphore_wait(barrier, gx_count - 1 + gy_count - 1 + 4)
        for side in range(2):
            col_copy(a, side).start()
        for vert in range(2):

            @pl.when(senders[vert])
            def _():
                row_copy(a, vert).start()

    shift = X0 - C0
    tmp[2, HALO : HALO + BY, 0:span] = damp_ref[...]
    frame[1] = pltpu.roll(tmp[2, 0:rows, :], shift, 1)

    def start_frames(kind):
        for side in range(2):
            side_copy(kind, side).start()
        for vert in range(2):

            @pl.when(senders[vert])
            def _():
                for column in range(3):
                    vert_copy(kind, vert, column).start()

    def wait_frames(kind):
        for side in range(2):
            side_copy(kind, side).wait()
        for vert in range(2):

            @pl.when(senders[vert])
            def _():
                for column in range(3):
                    vert_copy(kind, vert, column).wait_send()

            @pl.when(receivers[vert])
            def _():
                for column in range(3):
                    vert_copy(kind, vert, column).wait_recv()

    start_frames(1)

    halo_columns = ((X0 - HALO, X0), (X0 + span, X0 + span + HALO))

    def put_columns():
        for a in range(2):
            for side, (lo, hi) in enumerate(halo_columns):
                for y in range(BY):
                    strip[a, HALO + y, lo:hi, :] = colrecv[side, a, y]

    def put_corners(vert):
        base = 0 if vert == 0 else HALO + BY
        for a in range(2):
            for side, (lo, hi) in enumerate(halo_columns):
                for y in range(HALO):
                    strip[a, base + y, lo:hi, :] = corner[vert, side, a, y]

    lane = lax.broadcasted_iota(jnp.int32, (8, 128), 1)
    low = lane < HALF
    level = jnp.where(low, lane, lane - HALF).astype(jnp.float32)

    def prepare(tiles, y, depths):
        kept = list(depths)
        for v in tiles:
            here = pl.ds(C0 + 8 * v, 8)
            flow = strip[0, y, here, :]
            depth = jnp.broadcast_to(flow[:, levels : levels + 1], (8, 128))
            mixing = jnp.broadcast_to(flow[:, HALF + levels : HALF + levels + 1], (8, 128))
            turned = pltpu.roll(flow, HALF, 1)
            w_[y, here, :] = jnp.where(level < depth, 1.0, 0.0)
            u_[y, here, :] = jnp.where(low, flow, turned)
            n_[y, here, :] = jnp.where(low, turned, flow)
            m_[y, here, :] = mixing_rate * mixing
            kept[v] = jnp.where(lane == y, depth, depths[v])
        return tuple(kept)

    blank = tuple(jnp.zeros((8, 128), jnp.float32) for _ in range(width_vregs))

    def faces(tiles, y, carry):
        for v in tiles:
            x = C0 + 8 * v
            here = pl.ds(x, 8)
            there = pl.ds(x + 1, 8)
            wet = w_[y, here, :]
            wet_e = wet * w_[y, there, :]
            wet_n = wet * w_[y + 1, here, :]
            we[y, here, :] = wet_e
            wn[y, here, :] = wet_n
            scale = advect_rate * 0.25
            ce[y, here, :] = (scale * wet_e) * (u_[y, here, :] + u_[y, there, :])
            cn[y, here, :] = (scale * wet_n) * (n_[y, here, :] + n_[y + 1, here, :])
        return carry

    def first(f, tiles, y, carry):
        for v in tiles:
            x = C0 + 8 * v
            here, right, left = pl.ds(x, 8), pl.ds(x + 1, 8), pl.ds(x - 1, 8)
            mid = f[y, here, :]
            lap = (
                we[y, here, :] * (f[y, right, :] - mid)
                + we[y, left, :] * (f[y, left, :] - mid)
                + wn[y, here, :] * (f[y + 1, here, :] - mid)
                + wn[y - 1, here, :] * (f[y - 1, here, :] - mid)
            )
            g_[y, here, :] = m_[y, here, :] * lap
        return carry

    def second(f, y, v):
        x = C0 + 8 * v
        here, right, left = pl.ds(x, 8), pl.ds(x + 1, 8), pl.ds(x - 1, 8)
        mid = f[y, here, :]
        gm = g_[y, here, :]
        flow = (
            ce[y, here, :] * (mid + f[y, right, :])
            - ce[y, left, :] * (mid + f[y, left, :])
            + cn[y, here, :] * (mid + f[y + 1, here, :])
            - cn[y - 1, here, :] * (mid + f[y - 1, here, :])
        )
        mix = (
            we[y, here, :] * (g_[y, right, :] - gm)
            + we[y, left, :] * (g_[y, left, :] - gm)
            + wn[y, here, :] * (g_[y + 1, here, :] - gm)
            + wn[y - 1, here, :] * (g_[y - 1, here, :] - gm)
        )
        return mid - (flow + mix)

    old, new = strip.at[1], adv

    def pass_one(tiles, y, carry):
        for v in tiles:
            adv[y, pl.ds(C0 + 8 * v, 8), :] = second(old, y, v)
        return carry

    every = range(width_vregs)

    def early(step, bounds, tiles, carry=0):
        return lax.fori_loop(bounds[0], bounds[1], functools.partial(step, tiles), carry)

    def late(step, outer, bounds, tiles, carry=0):
        rest = [v for v in every if v not in tiles]
        carry = lax.fori_loop(outer[0], bounds[0], functools.partial(step, every), carry)
        carry = lax.fori_loop(bounds[1], outer[1], functools.partial(step, every), carry)
        return lax.fori_loop(bounds[0], bounds[1], functools.partial(step, rest), carry)

    last = rows - HALO
    full = span // 8
    step_one = functools.partial(first, old)
    depth_columns = early(prepare, (HALO, last), range(1, full + 1), blank)
    early(faces, (HALO, last - 1), range(1, full))
    for a in range(2):
        for side in range(2):
            col_copy(a, side).wait()
    for vert in range(2):

        @pl.when(senders[vert])
        def _():
            for side in range(2):
                corner_copy(vert, side).start()

    early(step_one, (HALO + 1, last - 1), range(2, full))
    early(pass_one, (HALO + 2, last - 2), range(3, full - 1))

    for vert in range(2):

        @pl.when(senders[vert])
        def _():
            for a in range(2):
                row_copy(a, vert).wait_send()
            for side in range(2):
                corner_copy(vert, side).wait_send()

        @pl.when(receivers[vert])
        def _():
            for a in range(2):
                row_copy(a, vert).wait_recv()
            for side in range(2):
                corner_copy(vert, side).wait_recv()

    put_columns()
    for vert in range(2):

        @pl.when(receivers[vert])
        def _():
            put_corners(vert)

    depth_columns = late(prepare, (0, rows), (HALO, last), range(1, full + 1), depth_columns)

    lanes = lax.broadcasted_iota(jnp.int32, (rows, 128), 1)
    ys = lax.broadcasted_iota(jnp.int32, (rows, 128), 0)
    sub = lax.broadcasted_iota(jnp.int32, (8, 128), 0)
    inside = (ys >= HALO) & (ys < HALO + BY) & (lanes >= shift) & (lanes < shift + span)

    def nbr_e(v):
        return pltpu.roll(v, 127, 1)

    def nbr_w(v):
        return pltpu.roll(v, 1, 1)

    def nbr_n(v):
        return pltpu.roll(v, rows - 1, 0)

    def nbr_s(v):
        return pltpu.roll(v, 1, 0)

    hops = (nbr_e, nbr_w, nbr_n, nbr_s)

    def to_grid(columns, t):
        for v in range(width_vregs):
            tmp[t, 8 * v : 8 * v + 8, :] = columns[v]
        if width_vregs < 16:
            tmp[t, 8 * width_vregs : 128, :] = jnp.zeros((128 - 8 * width_vregs, 128), jnp.float32)
        return tmp[t].T[0:rows, :]

    def pack(products):
        columns = [jnp.sum(jnp.where(inside, p, 0.0), axis=0, keepdims=True) for p in products]
        row = jnp.zeros((1, 128), jnp.float32)
        place = lax.broadcasted_iota(jnp.int32, (1, 128), 1)
        for k, column in enumerate(columns):
            row = jnp.where(place == k, jnp.sum(column, axis=1, keepdims=True), row)
        return row

    def x_copy(buffer, sems, k):
        return remote(buffer.at[0], buffer.at[k], sems, k, (lax.rem(gx + k, gx_count), gy))

    def y_copy(buffer, sems, k):
        return remote(buffer.at[0], buffer.at[k], sems, k, (gx, lax.rem(gy + k, gy_count)))

    def start_sum(copy, buffer, sems, row):
        buffer[0] = row
        for k in range(1, buffer.shape[0]):
            copy(buffer, sems, k).start()

    def end_sum(copy, buffer, sems):
        for k in range(1, buffer.shape[0]):
            copy(buffer, sems, k).wait()
        total = buffer[0]
        for k in range(1, buffer.shape[0]):
            total = total + buffer[k]
        return total

    depth_grid = to_grid(depth_columns, 1)
    couplings = [jnp.minimum(depth_grid, hop(depth_grid)) / levels for hop in hops]
    coupled = couplings[0] + couplings[1] + couplings[2] + couplings[3]
    squares = sum(c * c for c in couplings)
    own = frame[1] + coupled
    start_sum(
        x_copy, fitx, fitx_sem,
        pack([depth_grid, depth_grid * own, depth_grid * (own * own + squares)]),
    )

    late(faces, (0, rows - 1), (HALO, last - 1), range(1, full))
    late(step_one, (1, rows - 1), (HALO + 1, last - 1), range(2, full))
    late(pass_one, (2, rows - 2), (HALO + 2, last - 2), range(3, full - 1))
    start_sum(y_copy, fity, fity_sem, end_sum(x_copy, fitx, fitx_sem))
    lax.fori_loop(3, rows - 3, functools.partial(first, new, every), 0)
    weight = jnp.where(low, 1.0, -salt_weight) * (1.0 / math.sqrt(levels))

    def pass_two(y, sums):
        kept = []
        for v in range(width_vregs):
            here = pl.ds(C0 + 8 * v, 8)
            value = second(new, y, v)
            strip[1, y, here, :] = value
            total = jnp.sum(w_[y, here, :] * weight * value, axis=1, keepdims=True)
            kept.append(jnp.where(lane == y, jnp.broadcast_to(total, (8, 128)), sums[v]))
        return tuple(kept)

    forcing_columns = lax.fori_loop(HALO, HALO + BY, pass_two, blank)

    frame[0] = to_grid(forcing_columns, 0)
    start_frames(0)

    fit = end_sum(y_copy, fity, fity_sem)
    centre = fit[:, 1:2] / fit[:, 0:1]
    variance = fit[:, 2:3] / fit[:, 0:1] - centre * centre
    spread = jnp.maximum(2.0 * jnp.sqrt(jnp.maximum(variance, 0.0)), 0.1 * centre)
    centre = jnp.broadcast_to(centre, (1, 128))
    spread = jnp.broadcast_to(spread, (1, 128))

    for p in range(slots):
        for y in range(BY):
            cells[p, BX * y : BX * (y + 1), :] = strip[1, HALO + y, X0 + BX * p : X0 + BX * (p + 1), :]

    def give(cols, lanes, base):
        turned = [cells[p, pl.ds(base, 128), :].T for p in range(slots)]
        for s in range(slots):
            for n in range(2):
                value = tr_ref[s, n, :, cols]
                for p in range(slots):
                    piece = turned[p][HALF * n : HALF * n + levels, 0:lanes]
                    value = jnp.where(where_slot[s] == p, piece, value)
                out_v[s, n, :, cols] = value

    def give_chunk(j, carry):
        base = pl.multiple_of(j * 128, 128)
        give(pl.ds(base, 128), 128, base)
        return carry

    lax.fori_loop(0, chunks, give_chunk, 0)
    give(pl.ds(chunks * 128, tail), tail, chunks * 128)
    out_copy = pltpu.make_async_copy(out_v, out_ref, out_sem)
    out_copy.start()

    wait_frames(1)
    wait_frames(0)

    def extended(kind):
        parts = []
        for column, middle in enumerate((sideframe.at[0, kind], frame.at[kind], sideframe.at[1, kind])):
            south = jnp.where(has_s, vertframe[0, column, kind], 0.0)
            north = jnp.where(has_n, vertframe[1, column, kind], 0.0)
            first_rows = jnp.where(sub < HALO, south, middle[0:8, :])
            last_rows = jnp.where(sub < HALO, middle[rows - 8 : rows, :], north)
            parts.append(jnp.concatenate([first_rows, middle[8 : rows - 8, :], last_rows], axis=0))
        return jnp.where(
            lanes < shift,
            pltpu.roll(parts[0], 128 - span, 1),
            jnp.where(lanes < shift + span, parts[1], pltpu.roll(parts[2], span, 1)),
        )

    forcing = extended(0)
    damping = extended(1)

    diagonal = damping + coupled - centre

    def shifted(v):
        beside = [c * hop(v) for c, hop in zip(couplings, hops)]
        return (diagonal * v - (beside[0] + beside[1] + beside[2] + beside[3])) / spread

    basis = [forcing, shifted(forcing)]
    while len(basis) < ITERS + 1:
        basis.append(2.0 * shifted(basis[-1]) - basis[-2])
    pairs = ((0, 0), (0, 1), (1, 1), (1, 2), (2, 2), (2, 3), (0, 2), (0, 3), (1, 3))
    start_sum(x_copy, redx, redx_sem, pack([basis[i] * basis[j] for i, j in pairs]))
    start_sum(y_copy, redy, redy_sem, end_sum(x_copy, redx, redx_sem))
    total = end_sum(y_copy, redy, redy_sem)
    gram = {}
    for k, (i, j) in enumerate(pairs):
        gram[i, j] = gram[j, i] = jnp.broadcast_to(total[:, k : k + 1], (1, 128))

    def inner_product(a, b):
        value = None
        for i, ai in enumerate(a):
            for j, bj in enumerate(b):
                if ai is not None and bj is not None:
                    term = ai * bj * gram[i, j]
                    value = term if value is None else value + term
        return value

    def add(a, b):
        return b if a is None else a if b is None else a + b

    def combine(a, scale, b):
        return [add(ai, None if bi is None else scale * bi) for ai, bi in zip(a, b)]

    def image_of(p):
        image = [None] * (ITERS + 1)
        for i in range(ITERS):
            if p[i] is None:
                continue
            image[i] = add(image[i], centre * p[i])
            if i == 0:
                image[1] = add(image[1], spread * p[i])
            else:
                image[i + 1] = add(image[i + 1], (0.5 * spread) * p[i])
                image[i - 1] = add(image[i - 1], (0.5 * spread) * p[i])
        return image

    one = jnp.ones((1, 128), jnp.float32)
    residual = [one] + [None] * ITERS
    direction = [one] + [None] * ITERS
    height = [None] * (ITERS + 1)
    norm = gram[0, 0]
    for iteration in range(ITERS):
        image = image_of(direction)
        step = norm / inner_product(direction, image)
        height = combine(height, step, direction)
        if iteration + 1 < ITERS:
            residual = combine(residual, -step, image)
            norm_next = inner_product(residual, residual)
            direction = combine(residual, norm_next / norm, direction)
            norm = norm_next
    answer = height[0] * basis[0] + height[1] * basis[1] + height[2] * basis[2]
    answer = pltpu.roll(pltpu.roll(answer, 128 - shift, 1), rows - HALO, 0)
    sh_ref[...] = answer[0:BY, 0:span]
    out_copy.wait()


def per_device(block_list, wet_levels, mixing, velocity, tracers, damping):
    gx_count = lax.axis_size("gx")
    gy_count = lax.axis_size("gy")
    slots = tracers.shape[0]
    span = slots * BX
    rows = BY + 2 * HALO
    wide = -(-(X0 + span + HALO + 8) // 8) * 8
    f32 = jnp.float32
    big = pltpu.VMEM((rows, wide, 128), f32)
    vmem = pl.BlockSpec(memory_space=pltpu.VMEM)
    dma = pltpu.SemaphoreType.DMA
    cell_rows = -(-tracers.shape[3] // 128) * 128
    return pl.pallas_call(
        functools.partial(kernel, gx_count, gy_count),
        out_shape=(
            jax.ShapeDtypeStruct(tracers.shape, f32),
            jax.ShapeDtypeStruct(damping.shape, f32),
        ),
        in_specs=[pl.BlockSpec(memory_space=pltpu.SMEM)] + [vmem] * 5,
        out_specs=(pl.BlockSpec(memory_space=pl.ANY), vmem),
        scratch_shapes=[
            pltpu.VMEM((4, 128, 128), f32),
            pltpu.VMEM((4, cell_rows, 128), f32),
            pltpu.VMEM((2, rows, wide, 128), f32),
            big, big, big, big, big, big, big, big, big, big,
            pltpu.VMEM((2, 2, BY, HALO, 128), f32),
            pltpu.VMEM((2, 2, BY, HALO, 128), f32),
            pltpu.VMEM((2, 2, 2, HALO, HALO, 128), f32),
            pltpu.VMEM((2, rows, 128), f32),
            pltpu.VMEM((2, 2, rows, 128), f32),
            pltpu.VMEM((2, 3, 2, 8, 128), f32),
            pltpu.VMEM((gx_count, 1, 128), f32),
            pltpu.VMEM((gy_count, 1, 128), f32),
            pltpu.VMEM((gx_count, 1, 128), f32),
            pltpu.VMEM((gy_count, 1, 128), f32),
            pltpu.VMEM(tracers.shape, f32),
            dma((2, 4)), dma((2, 4)), dma((2, 4)), dma((2, 4)), dma((2, 12)),
            dma((2, gx_count)), dma((2, gy_count)), dma((2, gx_count)), dma((2, gy_count)), dma,
        ],
        compiler_params=pltpu.CompilerParams(
            collective_id=0, has_side_effects=True, vmem_limit_bytes=48 * 1024 * 1024
        ),
        name="ocean",
    )(block_list, wet_levels, mixing, velocity, tracers, damping)


def solution(mesh):
    return jax.shard_map(
        per_device,
        mesh=mesh,
        in_specs=(
            P(("gx", "gy")),
            P(("gx", "gy"), None),
            P(("gx", "gy"), None),
            P(("gx", "gy"), None, None, None),
            P(("gx", "gy"), None, None, None),
            P("gy", "gx"),
        ),
        out_specs=(P(("gx", "gy"), None, None, None), P("gy", "gx")),
        check_vma=False,
    )
```
